32 devices in a mesh: freq: 4 (over x, core), rec: 8 (over z, y).
Axes of the slice: x: 2, y: 2, z: 4, core: 2. Of those that a mesh axis runs over, the one named last changes fastest.
Arguments:
- response_real: float32 [96, 1536, 1536], P('freq', 'rec'), may hold values from -0.109375 to 0.109375
- response_imaginary: float32 [96, 1536, 1536], P('freq', 'rec'), may hold values from -0.109375 to 0.109375
- focus: float32 [1536, 96, 128], P('rec', 'freq'), may hold values from -6 to 6
- initial: float32 [1536, 96, 128], P('rec', 'freq'), may hold values from -6 to 6
- onset: int32 [1536, 64], P('rec'), may hold values from 24 to 167
Outputs:
- focus_next: float32 [1536, 96, 128], P('rec', 'freq')
The draws below stay inside these ranges and needn't reach their ends.
All inputs are finite; a program needn't handle non-finite values.
Results may differ from the reference program's by a relative error of at most 0.0003.
Values sent between devices are 32-bit elements; how exact they have to be, the bound alone decides.
A program may use at most 192 MiB of HBM per device.

```python
import math
import jax
import jax.numpy as jnp
from jax import lax

F = 96
NPOS = 1536
P_SIZE = 64
NT = 192


def set_ends(drawn, own_key, least, top_value):
    dims = drawn.shape
    place = [jax.random.randint(jax.random.fold_in(own_key, axis), (), 0, dims[axis]) for axis in range(len(dims))]
    drawn = drawn.at[tuple(place)].set(least)
    longest = dims.index(max(dims))
    place[longest] = (place[longest] + 1) % dims[longest]
    return drawn.at[tuple(place)].set(top_value)


def shard_levels(stream_key, shape, pieces, smallest, top_value):
    factor_of = 1.0
    for axis_at, blocks in pieces:
        steps = jax.random.uniform(jax.random.fold_in(jax.random.fold_in(stream_key, 6), axis_at), (blocks,), jnp.float32, smallest / len(pieces), top_value / len(pieces))
        factor_of = factor_of * jnp.repeat(jnp.exp(steps), shape[axis_at] // blocks).reshape((-1,) + (1,) * (len(shape) - 1 - axis_at))
    return factor_of


def scatter_about(stream_key, dims, spread, most, cuts=(), held_as=jnp.bfloat16):
    level = shard_levels(stream_key, dims, cuts, -0.22, 0.18) if cuts else 1.0
    values = jax.random.normal(stream_key, dims, jnp.float32) * spread * level
    return jnp.minimum(jnp.maximum(values, -most), most).astype(held_as)


def setup_inputs(seed: int = 0) -> dict:
    key_of = jax.random.split(jax.random.key(seed), 6)
    return {
        "response_real": scatter_about(key_of[0], (F, NPOS, NPOS), (2 * NPOS) ** -0.5, 0.109375, ((0, 4), (1, 8)), jnp.float32),
        "response_imaginary": scatter_about(key_of[1], (F, NPOS, NPOS), (2 * NPOS) ** -0.5, 0.109375, ((0, 4), (1, 8)), jnp.float32),
        "focus": scatter_about(key_of[2], (NPOS, F, 2 * P_SIZE), 1.0, 6.0, ((0, 8), (1, 4)), jnp.float32),
        "initial": scatter_about(key_of[3], (NPOS, F, 2 * P_SIZE), 1.0, 6.0, ((0, 8), (1, 4)), jnp.float32),
        "onset": set_ends(jax.random.randint(key_of[4], (NPOS, P_SIZE), NT // 8, NT - NT // 8), jax.random.fold_in(key_of[4], 1), NT // 8, (NT - NT // 8) - 1).astype(jnp.int32),
    }


def tables(freqs):
    samples = 2 * freqs
    order = lax.iota(jnp.int32, freqs)
    sample = lax.iota(jnp.int32, samples)
    phase = (order[:, None] * sample[None, :]) % samples
    phases = (2.0 * math.pi / samples) * phase.astype(jnp.float32)
    cosine = jnp.cos(phases)
    sine = jnp.sin(phases)
    factor = jnp.where(order == 0, 1.0, 2.0).astype(jnp.float32)[:, None] / samples
    inverse = jnp.stack([factor * cosine, -factor * sine])
    forward = jnp.stack([cosine, -sine])
    return inverse, forward, sample


def window(spectrum, onset):
    count, freqs, width = spectrum.shape
    half = width // 2
    inverse, forward, sample = tables(freqs)
    split = spectrum.reshape(count, freqs, 2, half)
    traces = jnp.einsum("nkcp,ckt->ntp", split, inverse, precision=lax.Precision.HIGHEST)
    keep = sample[None, :, None] < onset[:, None, :]
    clipped = jnp.where(keep, traces, 0.0)
    back = jnp.einsum("ntp,ckt->nkcp", clipped, forward, precision=lax.Precision.HIGHEST)
    return back.reshape(count, freqs, width)


def adjoint_terms(real_part, imag_part, values):
    half = values.shape[2] // 2
    first = jnp.einsum("frs,rfq->sfq", real_part, values, precision=lax.Precision.HIGHEST)
    second = jnp.einsum("frs,rfq->sfq", imag_part, values, precision=lax.Precision.HIGHEST)
    return jnp.concatenate([first[..., :half] + second[..., half:], first[..., half:] - second[..., :half]], axis=2)


def forward_terms(real_part, imag_part, values):
    half = values.shape[2] // 2
    first = jnp.einsum("frs,sfq->rfq", real_part, values, precision=lax.Precision.HIGHEST)
    second = jnp.einsum("frs,sfq->rfq", imag_part, values, precision=lax.Precision.HIGHEST)
    return jnp.concatenate([first[..., :half] - second[..., half:], first[..., half:] + second[..., :half]], axis=2)


def reference(response_real, response_imaginary, focus, initial, onset):
    adjoint = adjoint_terms(response_real, response_imaginary, focus)
    windowed = window(adjoint, onset)
    forward = forward_terms(response_real, response_imaginary, windowed)
    return initial - window(forward, onset)
```

```python
import functools
import math

import jax
import jax.numpy as jnp
import numpy as np
from jax import lax
from jax.experimental import pallas as pl
from jax.experimental.pallas import tpu as pltpu
from jax.sharding import PartitionSpec as P

CHUNKS = 4


class Ring:
    def __init__(self, total, size, stride):
        self.total, self.size, self.stride = total, size, stride

    def place(self):
        return lax.axis_index("rec") // self.stride % self.size

    def shift(self, x, by):
        pairs = []
        for index in range(self.total):
            own = index // self.stride % self.size
            moved = (own + by) % self.size
            pairs.append((index, index + (moved - own) * self.stride))
        return lax.ppermute(x, "rec", pairs)

    def gather(self, x, put, out):
        me, n = self.place(), self.size
        out = put(out, x, me)
        if n == 1:
            return out
        if n == 2:
            return put(out, self.shift(x, 1), (me + 1) % n)
        right = left = x
        for k in range(1, n // 2):
            right, left = self.shift(right, 1), self.shift(left, -1)
            out = put(out, right, (me + n - k) % n)
            out = put(out, left, (me + k) % n)
        cut = x.shape[0] // 2
        far = jnp.concatenate([self.shift(right[:cut], 1), self.shift(left[cut:], -1)], axis=0)
        return put(out, far, (me + n // 2) % n)

    def scatter(self, take):
        me, n = self.place(), self.size
        if n == 1:
            return take(me)
        if n == 2:
            return take(me) + self.shift(take((me + 1) % n), 1)
        far = take((me + n // 2) % n)
        cut = far.shape[0] // 2
        right, left = self.shift(far[:cut], 1), self.shift(far[cut:], -1)
        for k in range(n // 2 - 1, 0, -1):
            ahead, behind = take((me + k) % n), take((me + n - k) % n)
            if k == n // 2 - 1:
                right = jnp.concatenate([ahead[:cut] + right, ahead[cut:]], axis=0)
                left = jnp.concatenate([behind[:cut], behind[cut:] + left], axis=0)
            else:
                right, left = ahead + right, behind + left
            right, left = self.shift(right, 1), self.shift(left, -1)
        return take(me) + right + left


def rings():
    total = lax.axis_size("rec")
    inner = 1 << ((total.bit_length() - 1) // 2)
    if total % inner:
        inner = 1
    return Ring(total, total // inner, inner), Ring(total, inner, 1)


def scatter_sum(term, outer_first):
    outer, inner = rings()
    freqs, positions, width = term.shape
    count = positions // (outer.size * inner.size)
    blocks = term.reshape(freqs, outer.size, inner.size, count, width)
    dims = (1, 2) if outer_first else (2, 1)
    first, second = (outer, inner) if outer_first else (inner, outer)
    part = first.scatter(lambda at: lax.dynamic_index_in_dim(blocks, at, dims[0], keepdims=False))
    return second.scatter(lambda at: lax.dynamic_index_in_dim(part, at, 1, keepdims=False))


def gather_all(x, inner_first):
    outer, inner = rings()
    freqs, count, width = x.shape
    dims = (2, 1) if inner_first else (1, 2)
    first, second = (inner, outer) if inner_first else (outer, inner)

    def putter(dim):
        return lambda out, block, at: lax.dynamic_update_index_in_dim(out, block, at, dim)

    part = first.gather(x, putter(1), jnp.zeros((freqs, first.size, count, width), x.dtype))
    whole = jnp.zeros((freqs, outer.size, inner.size, count, width), x.dtype)
    whole = second.gather(part, putter(dims[1]), whole)
    return whole.reshape(freqs, -1, width)


def split_host(table):
    high = np.asarray(table, dtype=jnp.bfloat16)
    low = np.asarray(table - high.astype(np.float64), dtype=jnp.bfloat16)
    return high, low


def tables(freqs):
    samples = 2 * freqs
    order = np.arange(freqs)
    sample = np.arange(samples)
    phases = 2.0 * math.pi / samples * (order[:, None] * sample[None, :] % samples)
    cosine, sine = np.cos(phases), np.sin(phases)
    factor = np.where(order == 0, 1.0, 2.0)[:, None] / samples
    inverse = np.concatenate([(factor * cosine).T, (-factor * sine).T])
    forward = np.concatenate([cosine, -sine])
    return (*split_host(inverse), *split_host(forward))


def split(x):
    high = x.astype(jnp.bfloat16)
    return high, (x - high.astype(jnp.float32)).astype(jnp.bfloat16)


def product(high, low, x):
    x_high, x_low = split(x)
    dot = functools.partial(jnp.dot, preferred_element_type=jnp.float32)
    return dot(high, x_high) + (dot(high, x_low) + dot(low, x_high))


def window_kernel(onset_ref, ih_ref, il_ref, fh_ref, fl_ref, x_ref, o_ref):
    freqs, rows, width = x_ref.shape
    samples = 2 * freqs
    half = width // 2
    pair = 2
    lane = lax.broadcasted_iota(jnp.int32, (1, pair * width), 1) % width
    first = lane < half
    sample = lax.broadcasted_iota(jnp.int32, (samples, pair * width), 0)
    for i in range(0, rows, pair):
        x = jnp.concatenate([x_ref[:, i + j, :] for j in range(pair)], axis=1)
        both = product(ih_ref[...], il_ref[...], x)
        mixed = jnp.where(first, both[:samples], both[samples:])
        turned = jnp.concatenate(
            [pltpu.roll(mixed[:, j * width : (j + 1) * width], half, 1) for j in range(pair)], axis=1
        )
        onset = jnp.concatenate([onset_ref[i + j : i + j + 1, :] for j in range(pair)], axis=1)
        clipped = jnp.where(sample < onset, mixed + turned, 0.0)
        back = product(fh_ref[...], fl_ref[...], clipped)
        out = jnp.where(first, back[:freqs], back[freqs:])
        for j in range(pair):
            o_ref[:, i + j, :] = out[:, j * width : (j + 1) * width]


def window(spectrum, onset):
    freqs, count, width = spectrum.shape
    rows = 8 if count % 8 == 0 else count
    consts = [jnp.asarray(t) for t in tables(freqs)]
    whole = [pl.BlockSpec(t.shape, lambda i: (0, 0)) for t in consts]
    block = pl.BlockSpec((freqs, rows, width), lambda i: (0, i, 0))
    return pl.pallas_call(
        window_kernel,
        grid=(count // rows,),
        in_specs=[pl.BlockSpec((rows, width), lambda i: (i, 0)), *whole, block],
        out_specs=block,
        out_shape=jax.ShapeDtypeStruct(spectrum.shape, jnp.float32),
        name="window",
    )(onset, *consts, spectrum)


def onset_rows(onset):
    owned = onset.shape[0] // lax.axis_size("freq")
    mine = lax.dynamic_slice_in_dim(onset, lax.axis_index("freq") * owned, owned, 0)
    return jnp.concatenate([mine, mine], axis=1)


def einsum(form, a, b):
    return jnp.einsum(form, a, b, precision=lax.Precision.HIGH)


def on_device(response_real, response_imaginary, focus, initial, onset):
    freqs, _, _ = response_real.shape
    half = focus.shape[2] // 2
    local_onset = onset_rows(onset)
    step = freqs // CHUNKS
    pieces = [slice(c * step, (c + 1) * step) for c in range(CHUNKS)]
    values = jnp.swapaxes(focus, 0, 1)
    crossed = jnp.concatenate([values[..., half:], -values[..., :half]], axis=2)

    sums = []
    for number, piece in enumerate(pieces):
        term = einsum("frs,frq->fsq", response_real[piece], values[piece]) + einsum(
            "frs,frq->fsq", response_imaginary[piece], crossed[piece]
        )
        sums.append(scatter_sum(term, number == 0))
    partial_sum = jnp.concatenate(sums, axis=0)
    turned = lax.all_to_all(partial_sum, "freq", split_axis=1, concat_axis=0, tiled=True)
    windowed = window(turned, local_onset)
    returned = lax.all_to_all(windowed, "freq", split_axis=0, concat_axis=1, tiled=True)

    outs = []
    for number, piece in enumerate(pieces):
        full = gather_all(returned[piece], number == 0)
        turned_full = jnp.concatenate([-full[..., half:], full[..., :half]], axis=2)
        outs.append(
            einsum("frs,fsq->frq", response_real[piece], full)
            + einsum("frs,fsq->frq", response_imaginary[piece], turned_full)
        )
    forward = jnp.concatenate(outs, axis=0)
    receiver_side = lax.all_to_all(forward, "freq", split_axis=1, concat_axis=0, tiled=True)
    clipped = window(receiver_side, local_onset)
    update = lax.all_to_all(clipped, "freq", split_axis=0, concat_axis=1, tiled=True)
    return initial - jnp.swapaxes(update, 0, 1)


def solution(mesh):
    return jax.shard_map(
        on_device,
        mesh=mesh,
        in_specs=(
            P("freq", "rec", None),
            P("freq", "rec", None),
            P("rec", "freq", None),
            P("rec", "freq", None),
            P("rec", None),
        ),
        out_specs=P("rec", "freq", None),
        check_vma=False,
    )
```
